32 devices in a mesh: section: 2 (over core), expert: 16 (over z, y, x).
Axes of the slice: x: 2, y: 2, z: 4, core: 2. Of those that a mesh axis runs over, the one named last changes fastest.
Arguments:
- tokens: bfloat16 [2, 1024, 2048], P(None, 'expert'), may hold values from -6 to 6
- norm_gain: float32 [2, 2048], P('section'), may hold values from 0.5 to 2
- gate_weight: bfloat16 [2, 16, 2048, 768], P('section', 'expert'), may hold values from -0.125 to 0.125
- up_weight: bfloat16 [2, 16, 2048, 768], P('section', 'expert'), may hold values from -0.125 to 0.125
- down_weight: bfloat16 [2, 16, 768, 2048], P('section', 'expert'), may hold values from -0.21875 to 0.21875
- expert_place: int32 [2, 16], P('section'), may hold values from 0 to 15, each once within a row
- expert_ids: int32 [2, 2, 1024, 8], P('section', None, 'expert'), may hold values from 0 to 15, all different within a row; in each aligned block of 64 rows (0 to 63, 64 to 127, ..., all dimensions but the last counted through in order) at most 40 rows name the same one
- route_weights: float32 [2, 2, 1024, 8], P('section', None, 'expert'), may hold values from 0.05 to 0.4
Outputs:
- final_states: bfloat16 [2, 1024, 2048], P(None, 'expert')
The draws below stay inside these ranges and needn't reach their ends.
Inputs may be any that keep to these rules, and one draw needn't show every extreme that they name: `expert_ids`: each row names 8 different experts. In each aligned block of 64 rows (one device's tokens of one micro-batch in one layer) no expert is named by more than 40 rows, a bound that some block reaches. `expert_place`: each layer's row names every index along expert once.
All inputs are finite; a program needn't handle non-finite values.
Results may differ from the reference program's by a relative error of at most 0.013.
Values may be sent and summed in bfloat16 or wider, within the bound.
A program may use at most 128 MiB of HBM per device.

```python
import math
import jax
import jax.numpy as jnp
import numpy as np
from jax import lax

D = 2048
FFE = 768
TOPK = 8
MB = 2
TOK_DEV = 64
EXPERTS = 16
LAYERS = 2
TOKENS = 1024
CAP = 40
N_EXPERT = 16


def level_of(stream_key, dims, split, smallest, top_value):
    factor_of = 1.0
    for axis_at, parts in split:
        draws = jax.random.uniform(jax.random.fold_in(jax.random.fold_in(stream_key, 6), axis_at), (parts,), jnp.float32, smallest / len(split), top_value / len(split))
        factor_of = factor_of * jnp.repeat(jnp.exp(draws), dims[axis_at] // parts).reshape((-1,) + (1,) * (len(dims) - 1 - axis_at))
    return factor_of


def deal_out(own_key, own, number, rows, number_of, top, reach, lean):
    order = jax.random.permutation(own_key, number_of)
    crowded, common = portions_of(number_of, rows * top, reach, lean, True), portions_of(number_of, rows * top, reach, lean, False)
    places = jnp.arange(number_of)

    def named(lengths, rotation):
        used = int((lengths > 0).sum())
        fixed = max(1, used // 4)
        moved = fixed + (places - fixed + rotation * (used - fixed)) % max(1, number_of - fixed)
        return jnp.zeros((number_of,), jnp.int32).at[order[jnp.where(places < fixed, places, moved)]].set(jnp.asarray(lengths, jnp.int32))

    lengths = jnp.where(number % 4 == 0, named(crowded, number // 4), named(common, number - number // 4 - 1))
    mixed = jax.random.permutation(jax.random.fold_in(own, 3), number_of)
    source_of, sink = mixed[0:number_of // 2 * 2:2], mixed[1:number_of // 2 * 2:2]
    room = jnp.minimum(lengths[source_of] - 1, reach - lengths[sink]) // 2
    room = jnp.where((source_of == order[0]) | (sink == order[0]) | (lengths[sink] == 0), 0, jnp.maximum(room, 0))
    moved = jax.random.randint(jax.random.fold_in(own, 4), (number_of // 2,), 0, 1 << 20) % (room + 1)
    lengths = lengths.at[source_of].add(-moved).at[sink].add(moved)
    items = jnp.searchsorted(jnp.cumsum(lengths), jnp.arange(rows * top), side="right").astype(jnp.int32)
    table = items.reshape(top, rows).T
    table = table[jax.random.permutation(jax.random.fold_in(own, 1), rows)]
    rotation = jax.random.randint(jax.random.fold_in(own, 2), (rows, 1), 0, top)
    return jnp.take_along_axis(table, (jnp.arange(top)[None, :] + rotation) % top, axis=1)


def portions_of(number_of, total, limit, skew, full):
    weights = [(1 << 20) // math.isqrt(grade ** skew) + 1 for grade in range(1, number_of + 1)]
    largest = limit if full else min(limit, max(-(-total // number_of), total * weights[0] // sum(weights)))
    least = 1 if total - largest >= number_of - 1 else 0
    counts, spare = [largest] + [least] * (number_of - 1), total - largest - least * (number_of - 1)
    while spare > 0:
        candidates = [i for i in range(1, number_of) if counts[i] < largest] or [i for i in range(1, number_of) if counts[i] < limit]
        pool, left = sum([weights[i] for i in candidates]), spare
        for i in candidates:
            more = min(limit - counts[i], max(1, left * weights[i] // pool), spare)
            counts[i] = counts[i] + more
            spare = spare - more
    return np.array(counts)


def bell_draw(rng, extent, deviation, most, cuts=(), held_as=jnp.bfloat16):
    entries = deviation * jax.random.normal(rng, extent, jnp.float32)
    if cuts:
        entries = entries * level_of(rng, extent, cuts, -0.22, 0.18)
    return jnp.clip(entries, -most, most).astype(held_as)


def setup_inputs(seed: int = 0) -> dict:
    splits = jax.random.split(jax.random.key(seed), 9)
    tokens = bell_draw(splits[0], (MB, TOKENS, D), 1.0, 6.0, ((1, 16),))
    norm_gain = jnp.clip(jnp.exp(math.log(2.0) - 1.3862944 * jax.random.uniform(splits[1], (LAYERS, D), jnp.float32) ** level_of(splits[1], (LAYERS, D), ((0, 2),), -0.2, 0.2)), 0.5, 2.0)
    gate_weight = bell_draw(splits[2], (LAYERS, EXPERTS, D, FFE), D ** -0.5, 0.125, ((0, 2), (1, 16)))
    up_weight = bell_draw(splits[3], (LAYERS, EXPERTS, D, FFE), D ** -0.5, 0.125, ((0, 2), (1, 16)))
    down_weight = bell_draw(splits[4], (LAYERS, EXPERTS, FFE, D), FFE ** -0.5, 0.21875, ((0, 2), (1, 16)))
    expert_place = jax.vmap(lambda own: jax.random.permutation(own, EXPERTS))(jax.random.split(splits[5], LAYERS)).reshape((LAYERS, EXPERTS)).astype(jnp.int32)
    expert_ids_keys = jax.random.split(jax.random.fold_in(splits[6], 1), LAYERS * MB * TOKENS // TOK_DEV)
    expert_ids_turns = jax.random.permutation(jax.random.fold_in(splits[6], 3), LAYERS * MB * TOKENS // TOK_DEV)
    expert_ids = jax.vmap(lambda own, number: deal_out(jax.random.fold_in(splits[6], 2), own, number, TOK_DEV, EXPERTS, TOPK, CAP, 2))(expert_ids_keys, expert_ids_turns).reshape((LAYERS, MB, TOKENS, TOPK))
    route_weights = jnp.clip(0.05 + 0.35 * jax.random.uniform(splits[7], (LAYERS, MB, TOKENS, TOPK), jnp.float32) ** level_of(splits[7], (LAYERS, MB, TOKENS, TOPK), ((0, 2), (2, 16)), -0.2, 0.2), 0.05, 0.4)
    return dict(tokens=tokens, norm_gain=norm_gain, gate_weight=gate_weight, up_weight=up_weight, down_weight=down_weight, expert_place=expert_place, expert_ids=expert_ids, route_weights=route_weights)


EPSILON = 1e-06

def normalize(values, gain_row):
    widened = values.astype(jnp.float32)
    inverse_rms = lax.rsqrt(lax.optimization_barrier(jnp.mean(widened * widened, axis=-1, keepdims=True)) + EPSILON)
    return (widened * inverse_rms * gain_row[None, :]).astype(jnp.bfloat16)

def slot_positions(block_ids):
    onehot = (block_ids[..., None] == jnp.arange(EXPERTS, dtype=jnp.int32)).astype(jnp.int32)
    before = jnp.cumsum(onehot, axis=1) - onehot
    return lax.optimization_barrier(jnp.sum(before * onehot, axis=-1)).astype(jnp.int32)

def moe_layer(hidden, gain_row, gate_matrix, up_matrix, down_matrix, holder_table, chosen, weights):
    normed = normalize(hidden, gain_row)
    block_ids = chosen.reshape(N_EXPERT, TOK_DEV * TOPK)
    position = slot_positions(block_ids).reshape(-1)
    flat_ids = chosen.reshape(-1).astype(jnp.int32)
    entry_index = jnp.arange(TOKENS * TOPK, dtype=jnp.int32)
    source = entry_index // (TOK_DEV * TOPK)
    target = (flat_ids * N_EXPERT + source) * CAP + position
    token_row = entry_index // TOPK
    buffer = jnp.zeros((EXPERTS * N_EXPERT * CAP, D), jnp.bfloat16).at[target].set(normed[token_row])
    buffer = buffer.reshape(EXPERTS, N_EXPERT * CAP, D)

    def run_expert(expert):
        holder = holder_table[expert]
        row_block = buffer[expert]
        gate_part = jnp.dot(row_block, gate_matrix[holder], preferred_element_type=jnp.float32)
        up_part = jnp.dot(row_block, up_matrix[holder], preferred_element_type=jnp.float32)
        hidden_units = (jax.nn.silu(gate_part) * up_part).astype(jnp.bfloat16)
        return jnp.dot(hidden_units, down_matrix[holder], preferred_element_type=jnp.float32).astype(jnp.bfloat16)
    outputs = lax.map(run_expert, jnp.arange(EXPERTS, dtype=jnp.int32)).reshape(-1, D)
    picked = outputs[target].astype(jnp.float32).reshape(TOKENS, TOPK, D)
    mixture = jnp.einsum('tk,tkd->td', weights.astype(jnp.float32), picked)
    return (hidden.astype(jnp.float32) + mixture).astype(jnp.bfloat16)

def reference(tokens, norm_gain, gate_weight, up_weight, down_weight, expert_place, expert_ids, route_weights):
    finals = []
    for micro_index in range(MB):
        hidden = tokens[micro_index]
        for layer_index in range(LAYERS):
            hidden = moe_layer(hidden, norm_gain[layer_index], gate_weight[layer_index], up_weight[layer_index], down_weight[layer_index], expert_place[layer_index], expert_ids[layer_index, micro_index], route_weights[layer_index, micro_index])
        finals.append(hidden)
    return jnp.stack(finals)
```

```python
import functools

import jax
import jax.numpy as jnp
from jax import lax
from jax.experimental import pallas as pl
from jax.experimental.pallas import tpu as pltpu
from jax.sharding import PartitionSpec as P

EPSILON = 1e-06


def from_behind(array, axis, by):
    size = lax.axis_size(axis)
    return lax.ppermute(array, axis, [(i, (i + by) % size) for i in range(size)])


def normalize(values, gain_row):
    widened = values.astype(jnp.float32)
    inverse_rms = lax.rsqrt(jnp.mean(widened * widened, axis=-1, keepdims=True) + EPSILON)
    return (widened * inverse_rms * gain_row[None, :]).astype(jnp.bfloat16)


def expert_ffn(row_block, gate_matrix, up_matrix, down_matrix):
    gate_part = jnp.dot(row_block, gate_matrix, preferred_element_type=jnp.float32)
    up_part = jnp.dot(row_block, up_matrix, preferred_element_type=jnp.float32)
    hidden_units = (jax.nn.silu(gate_part) * up_part).astype(jnp.bfloat16)
    return jnp.dot(hidden_units, down_matrix, preferred_element_type=jnp.float32).astype(
        jnp.bfloat16
    )


def routed_local(
    tokens, norm_gain, gate_weight, up_weight, down_weight, expert_place, expert_ids, route_weights
):
    sections = lax.axis_size("section")
    groups = lax.axis_size("expert")
    section_index = lax.axis_index("section")
    micro_count = tokens.shape[0]
    tok_rows = tokens.shape[1]
    model_width = tokens.shape[2]
    top_count = expert_ids.shape[3]
    experts_all = expert_place.shape[1]
    capacity = max(2, 5 * tok_rows * top_count // (4 * experts_all))
    expert_lanes = jnp.arange(experts_all, dtype=jnp.int32)
    flat_token = jnp.arange(tok_rows * top_count, dtype=jnp.int32) // top_count
    own_params = (
        norm_gain[0],
        gate_weight[0, 0],
        up_weight[0, 0],
        down_weight[0, 0],
        expert_place[0],
        expert_ids[0],
        route_weights[0],
    )

    def run_rows(received, active, params):
        row_shape = received.shape
        flat_rows = received.reshape(-1, model_width)
        computed = lax.cond(
            active,
            lambda row_block: expert_ffn(row_block, params[1], params[2], params[3]),
            lambda row_block: jnp.zeros_like(row_block),
            flat_rows,
        )
        return computed.reshape(row_shape)

    def layer_step(hidden, micro_index, active, params):
        normed = normalize(hidden, params[0])
        holder_table = params[4]
        chosen = lax.dynamic_index_in_dim(params[5], micro_index, 0, keepdims=False).reshape(-1)
        weights = lax.dynamic_index_in_dim(params[6], micro_index, 0, keepdims=False)
        onehot = (chosen[:, None] == expert_lanes[None, :]).astype(jnp.int32)
        before = jnp.cumsum(onehot, axis=0) - onehot
        position = jnp.sum(before * onehot, axis=1)
        holder = jnp.sum(onehot * holder_table[None, :], axis=1)
        target = holder * capacity + position
        outgoing = (
            jnp.zeros((groups * capacity, model_width), jnp.bfloat16)
            .at[target]
            .set(normed[flat_token])
        )
        outgoing = outgoing.reshape(groups, capacity, model_width)
        received = lax.all_to_all(outgoing, "expert", split_axis=0, concat_axis=0, tiled=True)
        returned_rows = lax.all_to_all(
            run_rows(received, active, params), "expert", split_axis=0, concat_axis=0, tiled=True
        )
        picked = returned_rows.reshape(groups * capacity, model_width)[target]
        picked = picked.astype(jnp.float32).reshape(tok_rows, top_count, model_width)
        mixture = jnp.einsum("tk,tkd->td", weights, picked)
        return (hidden.astype(jnp.float32) + mixture).astype(jnp.bfloat16)

    other_mats = from_behind((own_params[1], own_params[2], own_params[3]), "section", 1)
    other_ints = from_behind((own_params[4], own_params[5]), "section", 1)
    other_floats = from_behind((own_params[0], own_params[6]), "section", 1)
    other_params = (
        other_floats[0],
        other_mats[0],
        other_mats[1],
        other_mats[2],
        other_ints[0],
        other_ints[1],
        other_floats[1],
    )
    is_first = section_index == 0
    first_params = tuple(
        (jnp.where(is_first, mine, theirs) for mine, theirs in zip(own_params, other_params))
    )
    second_params = tuple(
        (jnp.where(is_first, theirs, mine) for mine, theirs in zip(own_params, other_params))
    )
    share = micro_count // sections
    always = jnp.array(True)
    micro_index = section_index * share + 0
    hidden = lax.dynamic_index_in_dim(tokens, micro_index, 0, keepdims=False)
    hidden = layer_step(hidden, micro_index, always, first_params)
    hidden = layer_step(hidden, micro_index, always, second_params)
    own_finals = [hidden]
    return lax.all_gather(jnp.stack(own_finals), "section", axis=0, tiled=True)


def cascade_kernel(
    depth,
    cap,
    tokens_ref,
    gain_ref,
    dense_ref,
    gate_hbm,
    up_hbm,
    down_hbm,
    out_ref,
    gate_mats,
    up_mats,
    down_mats,
    other_gain,
    other_dense,
    meta,
    blocks,
    picks,
    held,
    outs,
    rets,
    sums,
    homes,
    hidden_ref,
    finals,
    core_sends,
    core_arrivals,
    meta_sends,
    meta_arrivals,
    block_sends,
    block_arrivals,
    pick_sends,
    pick_arrivals,
    ret_sends,
    ret_arrivals,
    home_sends,
    home_arrivals,
):
    section = lax.axis_index("section")
    me = lax.axis_index("expert")
    level = me // 4
    plane = lax.rem(me, 4)
    x_at = lax.rem(plane, 2)
    y_at = plane // 2
    rows, width = hidden_ref.shape
    groups = 4 * depth

    def at_level(offset):
        return lax.rem(level + offset + depth, depth) * 4 + plane

    def beside(j):
        x_to = 1 - x_at if j % 2 else x_at
        y_to = 1 - y_at if j // 2 else y_at
        return y_to * 2 + x_to

    def in_plane(j):
        return level * 4 + beside(j)

    barrier = pltpu.get_barrier_semaphore()
    partners = [{"section": 1 - section}]
    partners += [{"expert": at_level(k)} for k in range(1, depth)]
    partners += [{"expert": in_plane(j)} for j in range(1, 4)]
    for partner in partners:
        pl.semaphore_signal(
            barrier, inc=1, device_id=partner, device_id_type=pl.DeviceIdType.MESH
        )
    pl.semaphore_wait(barrier, len(partners))

    started = []

    def send(source, target, send_sem, arrival_sem, **peer):
        copy = pltpu.make_async_remote_copy(
            src_ref=source,
            dst_ref=target,
            send_sem=send_sem,
            recv_sem=arrival_sem,
            device_id=peer,
            device_id_type=pl.DeviceIdType.MESH,
        )
        copy.start()
        started.append(copy)
        return copy

    def to_core(i, source, target):
        return send(source, target, core_sends.at[i], core_arrivals.at[i], section=1 - section)

    gain_copy = to_core(0, gain_ref, other_gain)
    dense_copy = to_core(1, dense_ref.at[1 - section], other_dense)
    mats = [(gate_hbm, gate_mats), (up_hbm, up_mats), (down_hbm, down_mats)]
    mat_copies = [
        to_core(2 + i, source, target.at[section]) for i, (source, target) in enumerate(mats)
    ]
    own_copies = [
        pltpu.make_async_copy(source, target.at[section], core_sends.at[6 + i])
        for i, (source, target) in enumerate(mats)
    ]
    for copy in own_copies:
        copy.start()

    hidden_ref[...] = tokens_ref[section].astype(jnp.float32)
    gain_copy.wait_recv()
    is_first = section == 0
    gains = [
        jnp.where(is_first, gain_ref[...], other_gain[...]),
        jnp.where(is_first, other_gain[...], gain_ref[...]),
    ]

    def normed(layer):
        values = hidden_ref[...]
        inverse_rms = lax.rsqrt(jnp.mean(values * values, axis=-1, keepdims=True) + EPSILON)
        return (values * inverse_rms * gains[layer]).astype(jnp.bfloat16)

    row_at = lax.broadcasted_iota(jnp.int32, (rows, rows), 0)
    col_at = lax.broadcasted_iota(jnp.int32, (rows, rows), 1)
    earlier = jnp.where(col_at < row_at, 1.0, 0.0).astype(jnp.bfloat16)
    lane_of = lax.broadcasted_iota(jnp.int32, (rows, 128), 1)
    key_row = lax.broadcasted_iota(jnp.int32, (8, 128), 0)
    key_lane = lax.broadcasted_iota(jnp.int32, (8, 128), 1)

    for layer in range(2):
        blocks[layer, 0] = normed(layer)
        by_z = [None] + [
            send(
                blocks.at[layer, 0],
                blocks.at[layer, k],
                block_sends.at[layer, k],
                block_arrivals.at[layer, k],
                expert=at_level(k),
            )
            for k in range(1, depth)
        ]
        if layer == 0:
            dense_copy.wait_recv()
            meta[0] = dense_ref[section] + other_dense[...]
            meta_copies = [None] + [
                send(
                    meta.at[0],
                    meta.at[k],
                    meta_sends.at[k],
                    meta_arrivals.at[k],
                    expert=at_level(k),
                )
                for k in range(1, depth)
            ]
        lanes = [layer * groups + level * 4 + beside(j) for j in range(4)]
        picked, returned, homeward = {}, {}, {}

        def slots(k):
            chosen = meta[k] > 0.0
            flags = jnp.where(chosen, 1.0, 0.0).astype(jnp.bfloat16)
            before = jnp.dot(earlier, flags, preferred_element_type=jnp.float32)
            return jnp.where(chosen, before, -512.0)

        def select(k):
            if k:
                by_z[k].wait_recv()
                if layer == 0:
                    meta_copies[k].wait_recv()
            keys = jnp.zeros((8, 128), jnp.float32)
            for j in range(4):
                keys = jnp.where((key_row == j) & (key_lane == lanes[j]), 1.0, keys)
            across = lax.dot_general(
                keys.astype(jnp.bfloat16),
                slots(k).astype(jnp.bfloat16),
                (((1,), (1,)), ((), ())),
                preferred_element_type=jnp.float32,
            )
            slot_at = lax.broadcasted_iota(jnp.int32, (4 * cap, rows), 0).astype(jnp.float32)
            hits = jnp.zeros((4 * cap, rows), jnp.float32)
            for j in range(4):
                hits = jnp.where(slot_at == across[j : j + 1, :] + float(j * cap), 1.0, hits)
            taken = jnp.dot(
                hits.astype(jnp.bfloat16), blocks[layer, k], preferred_element_type=jnp.float32
            ).astype(jnp.bfloat16)
            for j in range(1, 4):
                picks[layer, k, j] = taken[j * cap : (j + 1) * cap]
                picked[k, j] = send(
                    picks.at[layer, k, j],
                    held.at[layer, k, j],
                    pick_sends.at[layer, k, j],
                    pick_arrivals.at[layer, k, j],
                    expert=in_plane(j),
                )
            held[layer, k, 0] = taken[0:cap]

        def compute(k):
            for j in range(1, 4):
                picked[k, j].wait_recv()
            block = held[layer, k].reshape(4 * cap, width)
            gate_part = jnp.dot(block, gate_mats[layer], preferred_element_type=jnp.float32)
            up_part = jnp.dot(block, up_mats[layer], preferred_element_type=jnp.float32)
            hidden_units = (gate_part / (1.0 + jnp.exp(-gate_part)) * up_part).astype(
                jnp.bfloat16
            )
            out = jnp.dot(hidden_units, down_mats[layer], preferred_element_type=jnp.float32)
            out = out.astype(jnp.bfloat16)
            for j in range(1, 4):
                outs[layer, k, j] = out[j * cap : (j + 1) * cap]
                returned[k, j] = send(
                    outs.at[layer, k, j],
                    rets.at[layer, k, j],
                    ret_sends.at[layer, k, j],
                    ret_arrivals.at[layer, k, j],
                    expert=in_plane(j),
                )
            rets[layer, k, 0] = out[0:cap]

        def combine(k):
            for j in range(1, 4):
                returned[k, j].wait_recv()
            place = slots(k)
            weights = meta[k]
            slot_at = lax.broadcasted_iota(jnp.int32, (rows, 4 * cap), 1).astype(jnp.float32)
            spread = jnp.zeros((rows, 4 * cap), jnp.float32)
            for j in range(4):
                named = lane_of == lanes[j]
                slot = jnp.sum(jnp.where(named, place, 0.0), axis=1, keepdims=True)
                weight = jnp.sum(jnp.where(named, weights, 0.0), axis=1, keepdims=True)
                spread = jnp.where(slot_at == slot + float(j * cap), weight, spread)
            high = spread.astype(jnp.bfloat16)
            low = (spread - high.astype(jnp.float32)).astype(jnp.bfloat16)
            both = jnp.dot(
                jnp.concatenate([high, low], axis=0),
                rets[layer, k].reshape(4 * cap, width),
                preferred_element_type=jnp.float32,
            )
            return both[0:rows] + both[rows:]

        def combine_home(k):
            sums[layer, k] = combine(k).astype(jnp.bfloat16)
            homeward[k] = send(
                sums.at[layer, k],
                homes.at[layer, k],
                home_sends.at[layer, k],
                home_arrivals.at[layer, k],
                expert=at_level(-k),
            )

        for k in range(depth):
            select(k)
        if layer == 0:
            for copy in own_copies:
                copy.wait()
            for copy in mat_copies:
                copy.wait_recv()
        for k in range(1, depth):
            compute(k)
        compute(0)
        for k in range(1, depth):
            combine_home(k)
        mixture = combine(0)
        for k in range(1, depth):
            homeward[k].wait_recv()
            mixture = mixture + homes[layer, k].astype(jnp.float32)
        hidden = (hidden_ref[...] + mixture).astype(jnp.bfloat16)
        if layer == 0:
            hidden_ref[...] = hidden.astype(jnp.float32)
        else:
            finals[0] = hidden

    final_copy = to_core(5, finals.at[0], finals.at[1])
    out_ref[section] = finals[0]
    final_copy.wait_recv()
    out_ref[1 - section] = finals[1]
    for copy in started:
        copy.wait_send()


def cascade_call(tokens, gain, dense, gate_matrix, up_matrix, down_matrix, depth, cap):
    rows, width = tokens.shape[1:]
    vmem = pl.BlockSpec(memory_space=pltpu.VMEM)
    anywhere = pl.BlockSpec(memory_space=pl.ANY)
    bf16, f32 = jnp.bfloat16, jnp.float32
    sems = pltpu.SemaphoreType.DMA
    return pl.pallas_call(
        functools.partial(cascade_kernel, depth, cap),
        out_shape=jax.ShapeDtypeStruct((2, rows, width), bf16),
        in_specs=[vmem, vmem, vmem, anywhere, anywhere, anywhere],
        out_specs=vmem,
        scratch_shapes=[
            pltpu.VMEM((2,) + gate_matrix.shape, bf16),
            pltpu.VMEM((2,) + up_matrix.shape, bf16),
            pltpu.VMEM((2,) + down_matrix.shape, bf16),
            pltpu.VMEM(gain.shape, f32),
            pltpu.VMEM(dense.shape[1:], f32),
            pltpu.VMEM((depth,) + dense.shape[1:], f32),
            pltpu.VMEM((2, depth, rows, width), bf16),
            pltpu.VMEM((2, depth, 4, cap, width), bf16),
            pltpu.VMEM((2, depth, 4, cap, width), bf16),
            pltpu.VMEM((2, depth, 4, cap, width), bf16),
            pltpu.VMEM((2, depth, 4, cap, width), bf16),
            pltpu.VMEM((2, depth, rows, width), bf16),
            pltpu.VMEM((2, depth, rows, width), bf16),
            pltpu.VMEM((rows, width), f32),
            pltpu.VMEM((2, rows, width), bf16),
            sems((9,)),
            sems((6,)),
            sems((depth,)),
            sems((depth,)),
            sems((2, depth)),
            sems((2, depth)),
            sems((2, depth, 4)),
            sems((2, depth, 4)),
            sems((2, depth, 4)),
            sems((2, depth, 4)),
            sems((2, depth)),
            sems((2, depth)),
        ],
        compiler_params=pltpu.CompilerParams(
            collective_id=0,
            has_side_effects=True,
            vmem_limit_bytes=60 * 1024 * 1024,
        ),
    )(tokens, gain, dense, gate_matrix, up_matrix, down_matrix)


def dense_local(
    tokens, norm_gain, gate_weight, up_weight, down_weight, expert_place, expert_ids, route_weights
):
    groups = lax.axis_size("expert")
    section_index = lax.axis_index("section")
    tok_rows, top_count = expert_ids.shape[2:]
    cap = 5 * tok_rows * top_count // (4 * groups)
    experts = jnp.arange(groups, dtype=jnp.int32)
    held_by = jnp.sum(
        jnp.where(expert_ids[0][..., None] == experts, expert_place[0], 0), axis=-1
    )
    lanes = jnp.arange(128, dtype=jnp.int32) - groups * section_index
    dense = jnp.sum(
        jnp.where(held_by[..., None] == lanes, route_weights[0][..., None], 0.0), axis=2
    )
    return cascade_call(
        tokens,
        norm_gain,
        dense,
        gate_weight[0, 0],
        up_weight[0, 0],
        down_weight[0, 0],
        groups // 4,
        cap,
    )


def local(
    tokens, norm_gain, gate_weight, up_weight, down_weight, expert_place, expert_ids, route_weights
):
    dense = 2 * expert_ids.shape[3] >= expert_place.shape[1] and tokens.shape[0] == 2
    dense = dense and lax.axis_size("expert") % 4 == 0 and 4 < lax.axis_size("expert") <= 64
    run = dense_local if dense else routed_local
    return run(
        tokens,
        norm_gain,
        gate_weight,
        up_weight,
        down_weight,
        expert_place,
        expert_ids,
        route_weights,
    )


def solution(mesh):
    in_specs = (
        P(None, "expert", None),
        P("section", None),
        P("section", "expert", None, None),
        P("section", "expert", None, None),
        P("section", "expert", None, None),
        P("section", None),
        P("section", None, "expert", None),
        P("section", None, "expert", None),
    )
    out_specs = P(None, "expert", None)
    return jax.shard_map(local, mesh=mesh, in_specs=in_specs, out_specs=out_specs, check_vma=False)
```

```python
import functools

import jax
import jax.numpy as jnp
from jax import lax
from jax.experimental import pallas as pl
from jax.experimental.pallas import tpu as pltpu
from jax.sharding import PartitionSpec as P

EPSILON = 1e-06


def from_behind(array, axis, by):
    size = lax.axis_size(axis)
    return lax.ppermute(array, axis, [(i, (i + by) % size) for i in range(size)])


def normalize(values, gain_row):
    widened = values.astype(jnp.float32)
    inverse_rms = lax.rsqrt(jnp.mean(widened * widened, axis=-1, keepdims=True) + EPSILON)
    return (widened * inverse_rms * gain_row[None, :]).astype(jnp.bfloat16)


def expert_ffn(row_block, gate_matrix, up_matrix, down_matrix):
    gate_part = jnp.dot(row_block, gate_matrix, preferred_element_type=jnp.float32)
    up_part = jnp.dot(row_block, up_matrix, preferred_element_type=jnp.float32)
    hidden_units = (jax.nn.silu(gate_part) * up_part).astype(jnp.bfloat16)
    return jnp.dot(hidden_units, down_matrix, preferred_element_type=jnp.float32).astype(
        jnp.bfloat16
    )


def routed_local(
    tokens, norm_gain, gate_weight, up_weight, down_weight, expert_place, expert_ids, route_weights
):
    sections = lax.axis_size("section")
    groups = lax.axis_size("expert")
    section_index = lax.axis_index("section")
    micro_count = tokens.shape[0]
    tok_rows = tokens.shape[1]
    model_width = tokens.shape[2]
    top_count = expert_ids.shape[3]
    experts_all = expert_place.shape[1]
    capacity = max(2, 5 * tok_rows * top_count // (4 * experts_all))
    expert_lanes = jnp.arange(experts_all, dtype=jnp.int32)
    flat_token = jnp.arange(tok_rows * top_count, dtype=jnp.int32) // top_count
    own_params = (
        norm_gain[0],
        gate_weight[0, 0],
        up_weight[0, 0],
        down_weight[0, 0],
        expert_place[0],
        expert_ids[0],
        route_weights[0],
    )

    def run_rows(received, active, params):
        row_shape = received.shape
        flat_rows = received.reshape(-1, model_width)
        computed = lax.cond(
            active,
            lambda row_block: expert_ffn(row_block, params[1], params[2], params[3]),
            lambda row_block: jnp.zeros_like(row_block),
            flat_rows,
        )
        return computed.reshape(row_shape)

    def layer_step(hidden, micro_index, active, params):
        normed = normalize(hidden, params[0])
        holder_table = params[4]
        chosen = lax.dynamic_index_in_dim(params[5], micro_index, 0, keepdims=False).reshape(-1)
        weights = lax.dynamic_index_in_dim(params[6], micro_index, 0, keepdims=False)
        onehot = (chosen[:, None] == expert_lanes[None, :]).astype(jnp.int32)
        before = jnp.cumsum(onehot, axis=0) - onehot
        position = jnp.sum(before * onehot, axis=1)
        holder = jnp.sum(onehot * holder_table[None, :], axis=1)
        target = holder * capacity + position
        outgoing = (
            jnp.zeros((groups * capacity, model_width), jnp.bfloat16)
            .at[target]
            .set(normed[flat_token])
        )
        outgoing = outgoing.reshape(groups, capacity, model_width)
        received = lax.all_to_all(outgoing, "expert", split_axis=0, concat_axis=0, tiled=True)
        returned_rows = lax.all_to_all(
            run_rows(received, active, params), "expert", split_axis=0, concat_axis=0, tiled=True
        )
        picked = returned_rows.reshape(groups * capacity, model_width)[target]
        picked = picked.astype(jnp.float32).reshape(tok_rows, top_count, model_width)
        mixture = jnp.einsum("tk,tkd->td", weights, picked)
        return (hidden.astype(jnp.float32) + mixture).astype(jnp.bfloat16)

    other_mats = from_behind((own_params[1], own_params[2], own_params[3]), "section", 1)
    other_ints = from_behind((own_params[4], own_params[5]), "section", 1)
    other_floats = from_behind((own_params[0], own_params[6]), "section", 1)
    other_params = (
        other_floats[0],
        other_mats[0],
        other_mats[1],
        other_mats[2],
        other_ints[0],
        other_ints[1],
        other_floats[1],
    )
    is_first = section_index == 0
    first_params = tuple(
        (jnp.where(is_first, mine, theirs) for mine, theirs in zip(own_params, other_params))
    )
    second_params = tuple(
        (jnp.where(is_first, theirs, mine) for mine, theirs in zip(own_params, other_params))
    )
    share = micro_count // sections
    always = jnp.array(True)
    micro_index = section_index * share + 0
    hidden = lax.dynamic_index_in_dim(tokens, micro_index, 0, keepdims=False)
    hidden = layer_step(hidden, micro_index, always, first_params)
    hidden = layer_step(hidden, micro_index, always, second_params)
    own_finals = [hidden]
    return lax.all_gather(jnp.stack(own_finals), "section", axis=0, tiled=True)


def cascade_kernel(
    depth,
    cap,
    tokens_ref,
    gain_ref,
    dense_ref,
    gate_hbm,
    up_hbm,
    down_hbm,
    out_ref,
    gate_mats,
    up_mats,
    down_mats,
    other_gain,
    other_dense,
    meta,
    places,
    blocks,
    picks,
    held,
    outs,
    rets,
    sums,
    relays,
    homes,
    hidden_ref,
    finals,
    core_sends,
    core_arrivals,
    meta_sends,
    meta_arrivals,
    block_sends,
    block_arrivals,
    pick_sends,
    pick_arrivals,
    ret_sends,
    ret_arrivals,
    home_sends,
    home_arrivals,
    relay_arrivals,
):
    section = lax.axis_index("section")
    me = lax.axis_index("expert")
    level = me // 4
    plane = lax.rem(me, 4)
    x_at = lax.rem(plane, 2)
    y_at = plane // 2
    rows, width = hidden_ref.shape
    upper = level // 2
    outer = jnp.where(upper == 1, lax.rem(level, 2), 1 - lax.rem(level, 2))
    mate = level + 1 - 2 * lax.rem(level, 2)
    far_inner = 2 - upper
    far_outer = 3 - 3 * upper

    def at_level(z):
        return z * 4 + plane

    def beside(j):
        x_to = 1 - x_at if j % 2 else x_at
        y_to = 1 - y_at if j // 2 else y_at
        return y_to * 2 + x_to

    def in_plane(j):
        return level * 4 + beside(j)

    barrier = pltpu.get_barrier_semaphore()
    partners = [{"section": 1 - section}]
    partners += [{"expert": at_level(z)} for z in (mate, far_inner, far_outer)]
    partners += [{"expert": in_plane(j)} for j in range(1, 4)]
    for partner in partners:
        pl.semaphore_signal(
            barrier, inc=1, device_id=partner, device_id_type=pl.DeviceIdType.MESH
        )
    pl.semaphore_wait(barrier, len(partners))

    started, inner_only = [], []

    def remote(source, target, send_sem, arrival_sem, **peer):
        return pltpu.make_async_remote_copy(
            src_ref=source,
            dst_ref=target,
            send_sem=send_sem,
            recv_sem=arrival_sem,
            device_id=peer,
            device_id_type=pl.DeviceIdType.MESH,
        )

    def send(*ends, **peer):
        copy = remote(*ends, **peer)
        copy.start()
        started.append(copy)
        return copy

    def wait_for(target, arrival_sem):
        remote(target, target, arrival_sem, arrival_sem, expert=at_level(mate)).wait_recv()

    def to_core(i, source, target):
        return send(source, target, core_sends.at[i], core_arrivals.at[i], section=1 - section)

    gain_copy = to_core(0, gain_ref, other_gain)
    dense_copy = to_core(1, dense_ref.at[1 - section], other_dense)
    mats = [(gate_hbm, gate_mats), (up_hbm, up_mats), (down_hbm, down_mats)]
    mat_copies = [
        to_core(2 + i, source, target.at[section]) for i, (source, target) in enumerate(mats)
    ]
    own_copies = [
        pltpu.make_async_copy(source, target.at[section], core_sends.at[6 + i])
        for i, (source, target) in enumerate(mats)
    ]
    for copy in own_copies:
        copy.start()

    hidden_ref[...] = tokens_ref[section].astype(jnp.float32)
    dense_copy.wait_recv()
    meta[0] = dense_ref[section] + other_dense[...]
    meta_copies = [
        send(meta.at[0], meta.at[slot], meta_sends.at[i], meta_arrivals.at[slot], expert=at_level(z))
        for i, (z, slot) in enumerate(
            [(mate, 1), (far_inner, 2 + outer), (far_outer, 2 + outer)]
        )
    ]
    gain_copy.wait_recv()
    is_first = section == 0
    gains = [
        jnp.where(is_first, gain_ref[...], other_gain[...]),
        jnp.where(is_first, other_gain[...], gain_ref[...]),
    ]

    def normed(layer):
        values = hidden_ref[...]
        inverse_rms = lax.rsqrt(jnp.mean(values * values, axis=-1, keepdims=True) + EPSILON)
        return (values * inverse_rms * gains[layer]).astype(jnp.bfloat16)

    span = meta.shape[2]
    row_at = lax.broadcasted_iota(jnp.int32, (span, span), 0)
    col_at = lax.broadcasted_iota(jnp.int32, (span, span), 1)
    earlier = jnp.where(row_at < col_at, 1.0, 0.0).astype(jnp.bfloat16)
    slot_at = lax.broadcasted_iota(jnp.int32, (4 * cap, rows), 0).astype(jnp.float32)

    def place_slots(k):
        chosen = meta[k] > 0.0
        flags = jnp.where(chosen, 1.0, 0.0).astype(jnp.bfloat16)
        before = jnp.dot(flags, earlier, preferred_element_type=jnp.float32)
        places[k] = jnp.where(chosen, before, -512.0)

    def spread_over(k, layer, weighted):
        spread = jnp.zeros((4 * cap, rows), jnp.float32)
        for j in range(4):
            row = pl.ds(layer * 4 * depth + in_plane(j), 1)
            slot = places[k, row, 0:rows]
            value = meta[k, row, 0:rows] if weighted else 1.0
            spread = jnp.where(slot_at == slot + float(j * cap), value, spread)
        return spread

    for layer in range(2):
        blocks[layer, 0] = normed(layer)

        def block_copy(i, source, slot, z):
            return remote(
                blocks.at[layer, source],
                blocks.at[layer, slot],
                block_sends.at[layer, i],
                block_arrivals.at[layer, slot],
                expert=at_level(z),
            )

        for copy in (block_copy(0, 0, 1, mate), block_copy(1, 0, 2 + outer, far_inner)):
            copy.start()
            started.append(copy)
        picked, returned = {}, {}

        def block_arrived(k):
            wait_for(blocks.at[layer, k], block_arrivals.at[layer, k])
            if k >= 2:
                forward = block_copy(k, k, k, mate)
                inner_only.append(forward)
                pl.when(outer == 0)(forward.start)

        def select(k):
            if layer == 0:
                if k:
                    wait_for(meta.at[k], meta_arrivals.at[k])
                place_slots(k)
            if k:
                block_arrived(k)
            taken = jnp.dot(
                spread_over(k, layer, False).astype(jnp.bfloat16),
                blocks[layer, k],
                preferred_element_type=jnp.float32,
            ).astype(jnp.bfloat16)
            for j in range(1, 4):
                picks[layer, k, j] = taken[j * cap : (j + 1) * cap]
                picked[k, j] = send(
                    picks.at[layer, k, j],
                    held.at[layer, k, j],
                    pick_sends.at[layer, k, j],
                    pick_arrivals.at[layer, k, j],
                    expert=in_plane(j),
                )
            held[layer, k, 0] = taken[0:cap]

        def compute(k):
            for j in range(1, 4):
                picked[k, j].wait_recv()
            block = held[layer, k].reshape(4 * cap, width)
            gate_part = jnp.dot(block, gate_mats[layer], preferred_element_type=jnp.float32)
            up_part = jnp.dot(block, up_mats[layer], preferred_element_type=jnp.float32)
            hidden_units = (gate_part / (1.0 + jnp.exp(-gate_part)) * up_part).astype(
                jnp.bfloat16
            )
            out = jnp.dot(hidden_units, down_mats[layer], preferred_element_type=jnp.float32)
            out = out.astype(jnp.bfloat16)
            for j in range(1, 4):
                outs[layer, k, j] = out[j * cap : (j + 1) * cap]
                returned[k, j] = send(
                    outs.at[layer, k, j],
                    rets.at[layer, k, j],
                    ret_sends.at[layer, k, j],
                    ret_arrivals.at[layer, k, j],
                    expert=in_plane(j),
                )
            rets[layer, k, 0] = out[0:cap]

        def combine(k):
            for j in range(1, 4):
                returned[k, j].wait_recv()
            spread = spread_over(k, layer, True)
            high = spread.astype(jnp.bfloat16)
            low = (spread - high.astype(jnp.float32)).astype(jnp.bfloat16)
            both = lax.dot_general(
                jnp.concatenate([high, low], axis=1),
                rets[layer, k].reshape(4 * cap, width),
                (((0,), (0,)), ((), ())),
                preferred_element_type=jnp.float32,
            )
            return both[0:rows] + both[rows:]

        def send_home(k, target, arrival, z):
            copy = remote(
                sums.at[layer, k], target, home_sends.at[layer, k], arrival, expert=at_level(z)
            )
            copy.start()
            return copy

        def combine_far(k):
            part = combine(k)
            relay, arrival = relays.at[layer, k - 2], relay_arrivals.at[layer, k - 2]

            @pl.when(outer == 1)
            def _():
                sums[layer, k] = part.astype(jnp.bfloat16)
                send_home(k, relay, arrival, mate)

            @pl.when(outer == 0)
            def _():
                wait_for(relay, arrival)
                joined = part + relays[layer, k - 2].astype(jnp.float32)
                sums[layer, k] = joined.astype(jnp.bfloat16)
                z = far_inner if k == 2 else far_outer
                send_home(k, homes.at[layer, 1], home_arrivals.at[layer, 1], z)

        for k in range(depth):
            select(k)
        if layer == 0:
            for copy in own_copies:
                copy.wait()
            for copy in mat_copies:
                copy.wait_recv()
        for k in (2, 3, 1, 0):
            compute(k)
        combine_far(2)
        combine_far(3)
        sums[layer, 1] = combine(1).astype(jnp.bfloat16)
        started.append(send_home(1, homes.at[layer, 0], home_arrivals.at[layer, 0], mate))
        mixture = combine(0)
        for i in range(2):
            wait_for(homes.at[layer, i], home_arrivals.at[layer, i])
            mixture = mixture + homes[layer, i].astype(jnp.float32)
        hidden = (hidden_ref[...] + mixture).astype(jnp.bfloat16)
        if layer == 0:
            hidden_ref[...] = hidden.astype(jnp.float32)
        else:
            finals[0] = hidden

    final_copy = to_core(5, finals.at[0], finals.at[1])
    out_ref[section] = finals[0]
    final_copy.wait_recv()
    out_ref[1 - section] = finals[1]
    for layer in range(2):
        for k in (2, 3):
            done = home_sends.at[layer, k]
            started.append(remote(sums.at[layer, k], sums.at[layer, k], done, done, expert=at_level(mate)))
    for copy in started:
        copy.wait_send()

    @pl.when(outer == 0)
    def _():
        for copy in inner_only:
            copy.wait_send()


def cascade_call(tokens, gain, dense, gate_matrix, up_matrix, down_matrix, depth, cap):
    rows, width = tokens.shape[1:]
    vmem = pl.BlockSpec(memory_space=pltpu.VMEM)
    anywhere = pl.BlockSpec(memory_space=pl.ANY)
    bf16, f32 = jnp.bfloat16, jnp.float32
    sems = pltpu.SemaphoreType.DMA
    return pl.pallas_call(
        functools.partial(cascade_kernel, depth, cap),
        out_shape=jax.ShapeDtypeStruct((2, rows, width), bf16),
        in_specs=[vmem, vmem, vmem, anywhere, anywhere, anywhere],
        out_specs=vmem,
        scratch_shapes=[
            pltpu.VMEM((2,) + gate_matrix.shape, bf16),
            pltpu.VMEM((2,) + up_matrix.shape, bf16),
            pltpu.VMEM((2,) + down_matrix.shape, bf16),
            pltpu.VMEM(gain.shape, f32),
            pltpu.VMEM(dense.shape[1:], f32),
            pltpu.VMEM((depth,) + dense.shape[1:], f32),
            pltpu.VMEM((depth,) + dense.shape[1:], f32),
            pltpu.VMEM((2, depth, rows, width), bf16),
            pltpu.VMEM((2, depth, 4, cap, width), bf16),
            pltpu.VMEM((2, depth, 4, cap, width), bf16),
            pltpu.VMEM((2, depth, 4, cap, width), bf16),
            pltpu.VMEM((2, depth, 4, cap, width), bf16),
            pltpu.VMEM((2, depth, rows, width), bf16),
            pltpu.VMEM((2, 2, rows, width), bf16),
            pltpu.VMEM((2, 2, rows, width), bf16),
            pltpu.VMEM((rows, width), f32),
            pltpu.VMEM((2, rows, width), bf16),
            sems((9,)),
            sems((6,)),
            sems((depth,)),
            sems((depth,)),
            sems((2, depth)),
            sems((2, depth)),
            sems((2, depth, 4)),
            sems((2, depth, 4)),
            sems((2, depth, 4)),
            sems((2, depth, 4)),
            sems((2, depth)),
            sems((2, 2)),
            sems((2, 2)),
        ],
        compiler_params=pltpu.CompilerParams(
            collective_id=0,
            has_side_effects=True,
            vmem_limit_bytes=60 * 1024 * 1024,
        ),
    )(tokens, gain, dense, gate_matrix, up_matrix, down_matrix)


def dense_local(
    tokens, norm_gain, gate_weight, up_weight, down_weight, expert_place, expert_ids, route_weights
):
    groups = lax.axis_size("expert")
    section_index = lax.axis_index("section")
    tok_rows, top_count = expert_ids.shape[2:]
    cap = 5 * tok_rows * top_count // (4 * groups)
    experts = jnp.arange(groups, dtype=jnp.int32)
    held_by = jnp.sum(
        jnp.where(expert_ids[0][..., None] == experts, expert_place[0], 0), axis=-1
    )
    holders = jnp.arange(2 * groups, dtype=jnp.int32) - groups * section_index
    dense = jnp.sum(
        jnp.where(
            held_by[:, None] == holders[:, None, None], route_weights[0][:, None], 0.0
        ),
        axis=-1,
    )
    dense = jnp.pad(dense, ((0, 0), (0, 0), (0, -tok_rows % 128)))
    return cascade_call(
        tokens,
        norm_gain,
        dense,
        gate_weight[0, 0],
        up_weight[0, 0],
        down_weight[0, 0],
        groups // 4,
        cap,
    )


def local(
    tokens, norm_gain, gate_weight, up_weight, down_weight, expert_place, expert_ids, route_weights
):
    dense = 2 * expert_ids.shape[3] >= expert_place.shape[1] and tokens.shape[0] == 2
    dense = dense and lax.axis_size("expert") % 4 == 0 and lax.axis_size("expert") == 16
    run = dense_local if dense else routed_local
    return run(
        tokens,
        norm_gain,
        gate_weight,
        up_weight,
        down_weight,
        expert_place,
        expert_ids,
        route_weights,
    )


def solution(mesh):
    in_specs = (
        P(None, "expert", None),
        P("section", None),
        P("section", "expert", None, None),
        P("section", "expert", None, None),
        P("section", "expert", None, None),
        P("section", None),
        P("section", None, "expert", None),
        P("section", None, "expert", None),
    )
    out_specs = P(None, "expert", None)
    return jax.shard_map(local, mesh=mesh, in_specs=in_specs, out_specs=out_specs, check_vma=False)
```

```python
import functools

import jax
import jax.numpy as jnp
from jax import lax
from jax.experimental import pallas as pl
from jax.experimental.pallas import tpu as pltpu
from jax.sharding import PartitionSpec as P

EPSILON = 1e-06


def from_behind(array, axis, by):
    size = lax.axis_size(axis)
    return lax.ppermute(array, axis, [(i, (i + by) % size) for i in range(size)])


def normalize(values, gain_row):
    widened = values.astype(jnp.float32)
    inverse_rms = lax.rsqrt(jnp.mean(widened * widened, axis=-1, keepdims=True) + EPSILON)
    return (widened * inverse_rms * gain_row[None, :]).astype(jnp.bfloat16)


def expert_ffn(row_block, gate_matrix, up_matrix, down_matrix):
    gate_part = jnp.dot(row_block, gate_matrix, preferred_element_type=jnp.float32)
    up_part = jnp.dot(row_block, up_matrix, preferred_element_type=jnp.float32)
    hidden_units = (jax.nn.silu(gate_part) * up_part).astype(jnp.bfloat16)
    return jnp.dot(hidden_units, down_matrix, preferred_element_type=jnp.float32).astype(
        jnp.bfloat16
    )


def routed_local(
    tokens, norm_gain, gate_weight, up_weight, down_weight, expert_place, expert_ids, route_weights
):
    sections = lax.axis_size("section")
    groups = lax.axis_size("expert")
    section_index = lax.axis_index("section")
    micro_count = tokens.shape[0]
    tok_rows = tokens.shape[1]
    model_width = tokens.shape[2]
    top_count = expert_ids.shape[3]
    experts_all = expert_place.shape[1]
    capacity = max(2, 5 * tok_rows * top_count // (4 * experts_all))
    expert_lanes = jnp.arange(experts_all, dtype=jnp.int32)
    flat_token = jnp.arange(tok_rows * top_count, dtype=jnp.int32) // top_count
    own_params = (
        norm_gain[0],
        gate_weight[0, 0],
        up_weight[0, 0],
        down_weight[0, 0],
        expert_place[0],
        expert_ids[0],
        route_weights[0],
    )

    def run_rows(received, active, params):
        row_shape = received.shape
        flat_rows = received.reshape(-1, model_width)
        computed = lax.cond(
            active,
            lambda row_block: expert_ffn(row_block, params[1], params[2], params[3]),
            lambda row_block: jnp.zeros_like(row_block),
            flat_rows,
        )
        return computed.reshape(row_shape)

    def layer_step(hidden, micro_index, active, params):
        normed = normalize(hidden, params[0])
        holder_table = params[4]
        chosen = lax.dynamic_index_in_dim(params[5], micro_index, 0, keepdims=False).reshape(-1)
        weights = lax.dynamic_index_in_dim(params[6], micro_index, 0, keepdims=False)
        onehot = (chosen[:, None] == expert_lanes[None, :]).astype(jnp.int32)
        before = jnp.cumsum(onehot, axis=0) - onehot
        position = jnp.sum(before * onehot, axis=1)
        holder = jnp.sum(onehot * holder_table[None, :], axis=1)
        target = holder * capacity + position
        outgoing = (
            jnp.zeros((groups * capacity, model_width), jnp.bfloat16)
            .at[target]
            .set(normed[flat_token])
        )
        outgoing = outgoing.reshape(groups, capacity, model_width)
        received = lax.all_to_all(outgoing, "expert", split_axis=0, concat_axis=0, tiled=True)
        returned_rows = lax.all_to_all(
            run_rows(received, active, params), "expert", split_axis=0, concat_axis=0, tiled=True
        )
        picked = returned_rows.reshape(groups * capacity, model_width)[target]
        picked = picked.astype(jnp.float32).reshape(tok_rows, top_count, model_width)
        mixture = jnp.einsum("tk,tkd->td", weights, picked)
        return (hidden.astype(jnp.float32) + mixture).astype(jnp.bfloat16)

    other_mats = from_behind((own_params[1], own_params[2], own_params[3]), "section", 1)
    other_ints = from_behind((own_params[4], own_params[5]), "section", 1)
    other_floats = from_behind((own_params[0], own_params[6]), "section", 1)
    other_params = (
        other_floats[0],
        other_mats[0],
        other_mats[1],
        other_mats[2],
        other_ints[0],
        other_ints[1],
        other_floats[1],
    )
    is_first = section_index == 0
    first_params = tuple(
        (jnp.where(is_first, mine, theirs) for mine, theirs in zip(own_params, other_params))
    )
    second_params = tuple(
        (jnp.where(is_first, theirs, mine) for mine, theirs in zip(own_params, other_params))
    )
    share = micro_count // sections
    always = jnp.array(True)
    micro_index = section_index * share + 0
    hidden = lax.dynamic_index_in_dim(tokens, micro_index, 0, keepdims=False)
    hidden = layer_step(hidden, micro_index, always, first_params)
    hidden = layer_step(hidden, micro_index, always, second_params)
    own_finals = [hidden]
    return lax.all_gather(jnp.stack(own_finals), "section", axis=0, tiled=True)


def cascade_kernel(
    depth,
    cap,
    tokens_ref,
    gain_ref,
    dense_ref,
    gate_hbm,
    up_hbm,
    down_hbm,
    out_ref,
    gate_mats,
    up_mats,
    down_mats,
    other_gain,
    other_dense,
    meta,
    places,
    blocks,
    picks,
    held,
    outs,
    rets,
    sums,
    relays,
    homes,
    flats,
    flat_picks,
    flat_held,
    flat_outs,
    flat_rets,
    flat_sums,
    flat_homes,
    parts,
    hidden_ref,
    finals,
    core_sends,
    core_arrivals,
    meta_sends,
    meta_arrivals,
    block_sends,
    block_arrivals,
    pick_sends,
    pick_arrivals,
    ret_sends,
    ret_arrivals,
    home_sends,
    home_arrivals,
    relay_arrivals,
    flat_sends,
    flat_arrivals,
    flat_pick_sends,
    flat_pick_arrivals,
    flat_ret_sends,
    flat_ret_arrivals,
    flat_home_sends,
    flat_home_arrivals,
):
    section = lax.axis_index("section")
    me = lax.axis_index("expert")
    level = me // 4
    plane = lax.rem(me, 4)
    x_at = lax.rem(plane, 2)
    y_at = plane // 2
    rows, width = hidden_ref.shape
    main = blocks.shape[3]
    upper = level // 2
    outer = jnp.where(upper == 1, lax.rem(level, 2), 1 - lax.rem(level, 2))
    mate = level + 1 - 2 * lax.rem(level, 2)
    far_inner = 2 - upper
    far_outer = 3 - 3 * upper

    def at_level(z):
        return z * 4 + plane

    def beside(j):
        x_to = 1 - x_at if j % 2 else x_at
        y_to = 1 - y_at if j // 2 else y_at
        return y_to * 2 + x_to

    def in_plane(j):
        return level * 4 + beside(j)

    barrier = pltpu.get_barrier_semaphore()
    partners = [{"section": 1 - section}]
    partners += [{"expert": at_level(z)} for z in (mate, far_inner, far_outer)]
    partners += [{"expert": in_plane(j)} for j in range(1, 4)]
    for partner in partners:
        pl.semaphore_signal(
            barrier, inc=1, device_id=partner, device_id_type=pl.DeviceIdType.MESH
        )
    pl.semaphore_wait(barrier, len(partners))

    started, inner_only = [], []

    def remote(source, target, send_sem, arrival_sem, **peer):
        return pltpu.make_async_remote_copy(
            src_ref=source,
            dst_ref=target,
            send_sem=send_sem,
            recv_sem=arrival_sem,
            device_id=peer,
            device_id_type=pl.DeviceIdType.MESH,
        )

    def send(*ends, **peer):
        copy = remote(*ends, **peer)
        copy.start()
        started.append(copy)
        return copy

    def wait_for(target, arrival_sem):
        remote(target, target, arrival_sem, arrival_sem, expert=at_level(mate)).wait_recv()

    def to_core(i, source, target):
        return send(source, target, core_sends.at[i], core_arrivals.at[i], section=1 - section)

    gain_copy = to_core(0, gain_ref, other_gain)
    dense_copy = to_core(1, dense_ref.at[1 - section], other_dense)
    mats = [(gate_hbm, gate_mats), (up_hbm, up_mats), (down_hbm, down_mats)]
    mat_copies = [
        to_core(2 + i, source, target.at[section]) for i, (source, target) in enumerate(mats)
    ]
    own_copies = [
        pltpu.make_async_copy(source, target.at[section], core_sends.at[6 + i])
        for i, (source, target) in enumerate(mats)
    ]
    for copy in own_copies:
        copy.start()

    hidden_ref[...] = tokens_ref[section].astype(jnp.float32)
    dense_copy.wait_recv()
    meta[0] = dense_ref[section] + other_dense[...]
    z_slots = [(mate, 1), (far_inner, 2 + outer), (far_outer, 2 + outer)]
    for i, (z, slot) in enumerate(z_slots):
        send(meta.at[0], meta.at[slot], meta_sends.at[i], meta_arrivals.at[slot], expert=at_level(z))
    for j in range(1, 4):
        place = 3 + j
        send(
            meta.at[0],
            meta.at[place],
            meta_sends.at[place],
            meta_arrivals.at[place],
            expert=in_plane(j),
        )
    gain_copy.wait_recv()
    is_first = section == 0
    gains = [
        jnp.where(is_first, gain_ref[...], other_gain[...]),
        jnp.where(is_first, other_gain[...], gain_ref[...]),
    ]

    def normed(layer):
        values = hidden_ref[...]
        inverse_rms = lax.rsqrt(jnp.mean(values * values, axis=-1, keepdims=True) + EPSILON)
        return (values * inverse_rms * gains[layer]).astype(jnp.bfloat16)

    span = meta.shape[2]
    row_at = lax.broadcasted_iota(jnp.int32, (span, span), 0)
    col_at = lax.broadcasted_iota(jnp.int32, (span, span), 1)
    earlier = jnp.where(row_at < col_at, 1.0, 0.0).astype(jnp.bfloat16)
    slot_at = lax.broadcasted_iota(jnp.int32, (4 * cap, rows), 0).astype(jnp.float32)
    plane_experts = [in_plane(j) for j in range(4)]
    column_experts = [at_level(z) for z in (level, mate, far_inner, far_outer)]

    def place_slots(place):
        if place:
            wait_for(meta.at[place], meta_arrivals.at[place])
        chosen = meta[place] > 0.0
        flags = jnp.where(chosen, 1.0, 0.0).astype(jnp.bfloat16)
        before = jnp.dot(flags, earlier, preferred_element_type=jnp.float32)
        places[place] = jnp.where(chosen, before, -512.0)

    def spread_over(place, experts, layer, weighted):
        spread = jnp.zeros((4 * cap, rows), jnp.float32)
        for j, expert in enumerate(experts):
            row = pl.ds(layer * 4 * depth + expert, 1)
            slot = places[place, row, 0:rows]
            value = meta[place, row, 0:rows] if weighted else 1.0
            spread = jnp.where(slot_at == slot + float(j * cap), value, spread)
        return spread

    def take(place, experts, layer, block):
        return jnp.dot(
            spread_over(place, experts, layer, False).astype(jnp.bfloat16),
            block,
            preferred_element_type=jnp.float32,
        ).astype(jnp.bfloat16)

    def scatter(place, experts, layer, returned_rows):
        spread = spread_over(place, experts, layer, True)
        high = spread.astype(jnp.bfloat16)
        low = (spread - high.astype(jnp.float32)).astype(jnp.bfloat16)
        both = lax.dot_general(
            jnp.concatenate([high, low], axis=1),
            returned_rows.reshape(4 * cap, returned_rows.shape[-1]),
            (((0,), (0,)), ((), ())),
            preferred_element_type=jnp.float32,
        )
        return both[0:rows] + both[rows:]

    for layer in range(2):
        start = normed(layer)
        blocks[layer, 0] = start[:, 0:main]
        flats[layer, 0] = start[:, main:]

        def block_copy(i, source, slot, z):
            return remote(
                blocks.at[layer, source],
                blocks.at[layer, slot],
                block_sends.at[layer, i],
                block_arrivals.at[layer, slot],
                expert=at_level(z),
            )

        for copy in (block_copy(0, 0, 1, mate), block_copy(1, 0, 2 + outer, far_inner)):
            copy.start()
            started.append(copy)
        flat_copies = [None] + [
            send(
                flats.at[layer, 0],
                flats.at[layer, j],
                flat_sends.at[layer, j],
                flat_arrivals.at[layer, j],
                expert=in_plane(j),
            )
            for j in range(1, 4)
        ]
        picked, returned, flat_home = {}, {}, {}

        def block_arrived(k):
            wait_for(blocks.at[layer, k], block_arrivals.at[layer, k])

        def pass_on():
            forwards = [block_copy(k, k, k, mate) for k in (2, 3)]
            inner_only.extend(forwards)

            @pl.when(outer == 0)
            def _():
                for k, forward in zip((2, 3), forwards):
                    block_arrived(k)
                    forward.start()

        def select(k):
            if layer == 0:
                place_slots(k)
            if k == 1:
                block_arrived(k)
            if k >= 2:
                pl.when(outer == 1)(functools.partial(block_arrived, k))
            taken = take(k, plane_experts, layer, blocks[layer, k])
            for j in range(1, 4):
                picks[layer, k, j] = taken[j * cap : (j + 1) * cap]
                picked[k, j] = send(
                    picks.at[layer, k, j],
                    held.at[layer, k, j],
                    pick_sends.at[layer, k, j],
                    pick_arrivals.at[layer, k, j],
                    expert=in_plane(j),
                )
            held[layer, k, 0] = taken[0:cap]

        def select_flat(j):
            place = 3 + j if j else 0
            if j:
                if layer == 0:
                    place_slots(place)
                flat_copies[j].wait_recv()
            taken = take(place, column_experts, layer, flats[layer, j])
            for i, (z, slot) in enumerate(z_slots):
                flat_picks[layer, j, i] = taken[(i + 1) * cap : (i + 2) * cap]
                send(
                    flat_picks.at[layer, j, i],
                    flat_held.at[layer, slot, j],
                    flat_pick_sends.at[layer, j, i],
                    flat_pick_arrivals.at[layer, slot, j],
                    expert=at_level(z),
                )
            flat_held[layer, 0, j] = taken[0:cap]

        def compute(k):
            for j in range(1, 4):
                picked[k, j].wait_recv()
            if k:
                for j in range(4):
                    wait_for(flat_held.at[layer, k, j], flat_pick_arrivals.at[layer, k, j])
            block = held[layer, k].reshape(4 * cap, main)
            rest = flat_held[layer, k].reshape(4 * cap, width - main)

            def project(mats):
                return jnp.dot(
                    block, mats[layer, 0:main], preferred_element_type=jnp.float32
                ) + jnp.dot(rest, mats[layer, main:], preferred_element_type=jnp.float32)

            gate_part = project(gate_mats)
            up_part = project(up_mats)
            hidden_units = (gate_part / (1.0 + jnp.exp(-gate_part)) * up_part).astype(
                jnp.bfloat16
            )
            out = jnp.dot(hidden_units, down_mats[layer], preferred_element_type=jnp.float32)
            out = out.astype(jnp.bfloat16)
            for j in range(1, 4):
                outs[layer, k, j] = out[j * cap : (j + 1) * cap, 0:main]
                returned[k, j] = send(
                    outs.at[layer, k, j],
                    rets.at[layer, k, j],
                    ret_sends.at[layer, k, j],
                    ret_arrivals.at[layer, k, j],
                    expert=in_plane(j),
                )
            rets[layer, k, 0] = out[0:cap, 0:main]
            flat_out = out[:, main:].reshape(4, cap, width - main)
            if k:
                flat_outs[layer, k - 1] = flat_out
                z, slot = z_slots[k - 1]
                send(
                    flat_outs.at[layer, k - 1],
                    flat_rets.at[layer, slot],
                    flat_ret_sends.at[layer, k],
                    flat_ret_arrivals.at[layer, slot],
                    expert=at_level(z),
                )
            else:
                flat_rets[layer, 0] = flat_out

        def combine(k):
            for j in range(1, 4):
                returned[k, j].wait_recv()
            return scatter(k, plane_experts, layer, rets[layer, k])

        def combine_flat(j):
            place = 3 + j if j else 0
            return scatter(place, column_experts, layer, flat_rets[layer, :, j])

        def send_home(k, target, arrival, z):
            copy = remote(
                sums.at[layer, k], target, home_sends.at[layer, k], arrival, expert=at_level(z)
            )
            copy.start()
            return copy

        def combine_far(k):
            part = combine(k)

            @pl.when(outer == 1)
            def _():
                sums[layer, k] = part.astype(jnp.bfloat16)
                relay, arrival = relays.at[layer, k - 2], relay_arrivals.at[layer, k - 2]
                send_home(k, relay, arrival, mate)

            @pl.when(outer == 0)
            def _():
                parts[k - 2] = part

        def join_far(k):
            @pl.when(outer == 0)
            def _():
                wait_for(relays.at[layer, k - 2], relay_arrivals.at[layer, k - 2])
                joined = parts[k - 2] + relays[layer, k - 2].astype(jnp.float32)
                sums[layer, k] = joined.astype(jnp.bfloat16)
                z = far_inner if k == 2 else far_outer
                send_home(k, homes.at[layer, 1], home_arrivals.at[layer, 1], z)

        select(0)
        select(1)
        pass_on()
        select(2)
        select_flat(0)
        select_flat(1)
        select_flat(2)
        select_flat(3)
        select(3)
        if layer == 0:
            for copy in own_copies:
                copy.wait()
            for copy in mat_copies:
                copy.wait_recv()
        for k in (2, 3, 1, 0):
            compute(k)
        combine_far(2)
        combine_far(3)
        sums[layer, 1] = combine(1).astype(jnp.bfloat16)
        started.append(send_home(1, homes.at[layer, 0], home_arrivals.at[layer, 0], mate))
        for k in range(1, depth):
            wait_for(flat_rets.at[layer, k], flat_ret_arrivals.at[layer, k])
        for j in range(1, 4):
            flat_sums[layer, j] = combine_flat(j).astype(jnp.bfloat16)
            flat_home[j] = send(
                flat_sums.at[layer, j],
                flat_homes.at[layer, j],
                flat_home_sends.at[layer, j],
                flat_home_arrivals.at[layer, j],
                expert=in_plane(j),
            )
        join_far(2)
        flat_mixture = combine_flat(0)
        join_far(3)
        mixture = combine(0)
        for j in range(1, 4):
            flat_home[j].wait_recv()
            flat_mixture = flat_mixture + flat_homes[layer, j].astype(jnp.float32)
        for i in range(2):
            wait_for(homes.at[layer, i], home_arrivals.at[layer, i])
            mixture = mixture + homes[layer, i].astype(jnp.float32)
        mixed = jnp.concatenate([mixture, flat_mixture], axis=1)
        hidden = (hidden_ref[...] + mixed).astype(jnp.bfloat16)
        if layer == 0:
            hidden_ref[...] = hidden.astype(jnp.float32)
        else:
            finals[0] = hidden

    final_copy = to_core(5, finals.at[0], finals.at[1])
    out_ref[section] = finals[0]
    final_copy.wait_recv()
    out_ref[1 - section] = finals[1]
    for layer in range(2):
        for k in (2, 3):
            done = home_sends.at[layer, k]
            started.append(remote(sums.at[layer, k], sums.at[layer, k], done, done, expert=at_level(mate)))
    for copy in started:
        copy.wait_send()

    @pl.when(outer == 0)
    def _():
        for copy in inner_only:
            copy.wait_send()


def cascade_call(tokens, gain, dense, gate_matrix, up_matrix, down_matrix, depth, cap):
    rows, width = tokens.shape[1:]
    rest = width // 4 // 128 * 128
    main = width - rest
    vmem = pl.BlockSpec(memory_space=pltpu.VMEM)
    anywhere = pl.BlockSpec(memory_space=pl.ANY)
    bf16, f32 = jnp.bfloat16, jnp.float32
    sems = pltpu.SemaphoreType.DMA
    return pl.pallas_call(
        functools.partial(cascade_kernel, depth, cap),
        out_shape=jax.ShapeDtypeStruct((2, rows, width), bf16),
        in_specs=[vmem, vmem, vmem, anywhere, anywhere, anywhere],
        out_specs=vmem,
        scratch_shapes=[
            pltpu.VMEM((2,) + gate_matrix.shape, bf16),
            pltpu.VMEM((2,) + up_matrix.shape, bf16),
            pltpu.VMEM((2,) + down_matrix.shape, bf16),
            pltpu.VMEM(gain.shape, f32),
            pltpu.VMEM(dense.shape[1:], f32),
            pltpu.VMEM((depth + 3,) + dense.shape[1:], f32),
            pltpu.VMEM((depth + 3,) + dense.shape[1:], f32),
            pltpu.VMEM((2, depth, rows, main), bf16),
            pltpu.VMEM((2, depth, 4, cap, main), bf16),
            pltpu.VMEM((2, depth, 4, cap, main), bf16),
            pltpu.VMEM((2, depth, 4, cap, main), bf16),
            pltpu.VMEM((2, depth, 4, cap, main), bf16),
            pltpu.VMEM((2, depth, rows, main), bf16),
            pltpu.VMEM((2, 2, rows, main), bf16),
            pltpu.VMEM((2, 2, rows, main), bf16),
            pltpu.VMEM((2, 4, rows, rest), bf16),
            pltpu.VMEM((2, 4, depth - 1, cap, rest), bf16),
            pltpu.VMEM((2, depth, 4, cap, rest), bf16),
            pltpu.VMEM((2, depth - 1, 4, cap, rest), bf16),
            pltpu.VMEM((2, depth, 4, cap, rest), bf16),
            pltpu.VMEM((2, 4, rows, rest), bf16),
            pltpu.VMEM((2, 4, rows, rest), bf16),
            pltpu.VMEM((2, rows, main), f32),
            pltpu.VMEM((rows, width), f32),
            pltpu.VMEM((2, rows, width), bf16),
            sems((9,)),
            sems((6,)),
            sems((depth + 3,)),
            sems((depth + 3,)),
            sems((2, depth)),
            sems((2, depth)),
            sems((2, depth, 4)),
            sems((2, depth, 4)),
            sems((2, depth, 4)),
            sems((2, depth, 4)),
            sems((2, depth)),
            sems((2, 2)),
            sems((2, 2)),
            sems((2, 4)),
            sems((2, 4)),
            sems((2, 4, depth - 1)),
            sems((2, depth, 4)),
            sems((2, depth)),
            sems((2, depth)),
            sems((2, 4)),
            sems((2, 4)),
        ],
        compiler_params=pltpu.CompilerParams(
            collective_id=0,
            has_side_effects=True,
            vmem_limit_bytes=60 * 1024 * 1024,
        ),
    )(tokens, gain, dense, gate_matrix, up_matrix, down_matrix)


def dense_local(
    tokens, norm_gain, gate_weight, up_weight, down_weight, expert_place, expert_ids, route_weights
):
    groups = lax.axis_size("expert")
    section_index = lax.axis_index("section")
    tok_rows, top_count = expert_ids.shape[2:]
    cap = 5 * tok_rows * top_count // (4 * groups)
    experts = jnp.arange(groups, dtype=jnp.int32)
    held_by = jnp.sum(
        jnp.where(expert_ids[0][..., None] == experts, expert_place[0], 0), axis=-1
    )
    holders = jnp.arange(2 * groups, dtype=jnp.int32) - groups * section_index
    dense = jnp.sum(
        jnp.where(
            held_by[:, None] == holders[:, None, None], route_weights[0][:, None], 0.0
        ),
        axis=-1,
    )
    dense = jnp.pad(dense, ((0, 0), (0, 0), (0, -tok_rows % 128)))
    return cascade_call(
        tokens,
        norm_gain,
        dense,
        gate_weight[0, 0],
        up_weight[0, 0],
        down_weight[0, 0],
        groups // 4,
        cap,
    )


def local(
    tokens, norm_gain, gate_weight, up_weight, down_weight, expert_place, expert_ids, route_weights
):
    dense = 2 * expert_ids.shape[3] >= expert_place.shape[1] and tokens.shape[0] == 2
    dense = dense and lax.axis_size("expert") % 4 == 0 and lax.axis_size("expert") == 16
    run = dense_local if dense else routed_local
    return run(
        tokens,
        norm_gain,
        gate_weight,
        up_weight,
        down_weight,
        expert_place,
        expert_ids,
        route_weights,
    )


def solution(mesh):
    in_specs = (
        P(None, "expert", None),
        P("section", None),
        P("section", "expert", None, None),
        P("section", "expert", None, None),
        P("section", "expert", None, None),
        P("section", None),
        P("section", None, "expert", None),
        P("section", None, "expert", None),
    )
    out_specs = P(None, "expert", None)
    return jax.shard_map(local, mesh=mesh, in_specs=in_specs, out_specs=out_specs, check_vma=False)
```

```python
import functools

import jax
import jax.numpy as jnp
from jax import lax
from jax.experimental import pallas as pl
from jax.experimental.pallas import tpu as pltpu
from jax.sharding import PartitionSpec as P

EPSILON = 1e-06


def from_behind(array, axis, by):
    size = lax.axis_size(axis)
    return lax.ppermute(array, axis, [(i, (i + by) % size) for i in range(size)])


def normalize(values, gain_row):
    widened = values.astype(jnp.float32)
    inverse_rms = lax.rsqrt(jnp.mean(widened * widened, axis=-1, keepdims=True) + EPSILON)
    return (widened * inverse_rms * gain_row[None, :]).astype(jnp.bfloat16)


def expert_ffn(row_block, gate_matrix, up_matrix, down_matrix):
    gate_part = jnp.dot(row_block, gate_matrix, preferred_element_type=jnp.float32)
    up_part = jnp.dot(row_block, up_matrix, preferred_element_type=jnp.float32)
    hidden_units = (jax.nn.silu(gate_part) * up_part).astype(jnp.bfloat16)
    return jnp.dot(hidden_units, down_matrix, preferred_element_type=jnp.float32).astype(
        jnp.bfloat16
    )


def routed_local(
    tokens, norm_gain, gate_weight, up_weight, down_weight, expert_place, expert_ids, route_weights
):
    sections = lax.axis_size("section")
    groups = lax.axis_size("expert")
    section_index = lax.axis_index("section")
    micro_count = tokens.shape[0]
    tok_rows = tokens.shape[1]
    model_width = tokens.shape[2]
    top_count = expert_ids.shape[3]
    experts_all = expert_place.shape[1]
    capacity = max(2, 5 * tok_rows * top_count // (4 * experts_all))
    expert_lanes = jnp.arange(experts_all, dtype=jnp.int32)
    flat_token = jnp.arange(tok_rows * top_count, dtype=jnp.int32) // top_count
    own_params = (
        norm_gain[0],
        gate_weight[0, 0],
        up_weight[0, 0],
        down_weight[0, 0],
        expert_place[0],
        expert_ids[0],
        route_weights[0],
    )

    def run_rows(received, active, params):
        row_shape = received.shape
        flat_rows = received.reshape(-1, model_width)
        computed = lax.cond(
            active,
            lambda row_block: expert_ffn(row_block, params[1], params[2], params[3]),
            lambda row_block: jnp.zeros_like(row_block),
            flat_rows,
        )
        return computed.reshape(row_shape)

    def layer_step(hidden, micro_index, active, params):
        normed = normalize(hidden, params[0])
        holder_table = params[4]
        chosen = lax.dynamic_index_in_dim(params[5], micro_index, 0, keepdims=False).reshape(-1)
        weights = lax.dynamic_index_in_dim(params[6], micro_index, 0, keepdims=False)
        onehot = (chosen[:, None] == expert_lanes[None, :]).astype(jnp.int32)
        before = jnp.cumsum(onehot, axis=0) - onehot
        position = jnp.sum(before * onehot, axis=1)
        holder = jnp.sum(onehot * holder_table[None, :], axis=1)
        target = holder * capacity + position
        outgoing = (
            jnp.zeros((groups * capacity, model_width), jnp.bfloat16)
            .at[target]
            .set(normed[flat_token])
        )
        outgoing = outgoing.reshape(groups, capacity, model_width)
        received = lax.all_to_all(outgoing, "expert", split_axis=0, concat_axis=0, tiled=True)
        returned_rows = lax.all_to_all(
            run_rows(received, active, params), "expert", split_axis=0, concat_axis=0, tiled=True
        )
        picked = returned_rows.reshape(groups * capacity, model_width)[target]
        picked = picked.astype(jnp.float32).reshape(tok_rows, top_count, model_width)
        mixture = jnp.einsum("tk,tkd->td", weights, picked)
        return (hidden.astype(jnp.float32) + mixture).astype(jnp.bfloat16)

    other_mats = from_behind((own_params[1], own_params[2], own_params[3]), "section", 1)
    other_ints = from_behind((own_params[4], own_params[5]), "section", 1)
    other_floats = from_behind((own_params[0], own_params[6]), "section", 1)
    other_params = (
        other_floats[0],
        other_mats[0],
        other_mats[1],
        other_mats[2],
        other_ints[0],
        other_ints[1],
        other_floats[1],
    )
    is_first = section_index == 0
    first_params = tuple(
        (jnp.where(is_first, mine, theirs) for mine, theirs in zip(own_params, other_params))
    )
    second_params = tuple(
        (jnp.where(is_first, theirs, mine) for mine, theirs in zip(own_params, other_params))
    )
    share = micro_count // sections
    always = jnp.array(True)
    micro_index = section_index * share + 0
    hidden = lax.dynamic_index_in_dim(tokens, micro_index, 0, keepdims=False)
    hidden = layer_step(hidden, micro_index, always, first_params)
    hidden = layer_step(hidden, micro_index, always, second_params)
    own_finals = [hidden]
    return lax.all_gather(jnp.stack(own_finals), "section", axis=0, tiled=True)


def cascade_kernel(
    depth,
    cap,
    tokens_ref,
    gain_ref,
    place_ref,
    ids_ref,
    route_ref,
    gate_hbm,
    up_hbm,
    down_hbm,
    finals,
    gate_mats,
    up_mats,
    down_mats,
    other_gain,
    other_dense,
    meta,
    places,
    blocks,
    picks,
    held,
    outs,
    rets,
    sums,
    relays,
    homes,
    flats,
    flat_picks,
    flat_held,
    flat_outs,
    flat_rets,
    flat_sums,
    flat_homes,
    parts,
    hidden_ref,
    dense_ref,
    core_sends,
    core_arrivals,
    meta_sends,
    meta_arrivals,
    block_sends,
    block_arrivals,
    pick_sends,
    pick_arrivals,
    ret_sends,
    ret_arrivals,
    home_sends,
    home_arrivals,
    relay_arrivals,
    flat_sends,
    flat_arrivals,
    flat_pick_sends,
    flat_pick_arrivals,
    flat_ret_sends,
    flat_ret_arrivals,
    flat_home_sends,
    flat_home_arrivals,
):
    section = lax.axis_index("section")
    me = lax.axis_index("expert")
    level = me // 4
    plane = lax.rem(me, 4)
    x_at = lax.rem(plane, 2)
    y_at = plane // 2
    rows, width = hidden_ref.shape
    groups = 4 * depth
    main = blocks.shape[3]
    back = outs.shape[4]
    upper = level // 2
    outer = jnp.where(upper == 1, lax.rem(level, 2), 1 - lax.rem(level, 2))
    mate = level + 1 - 2 * lax.rem(level, 2)
    far_inner = 2 - upper
    far_outer = 3 - 3 * upper

    def at_level(z):
        return z * 4 + plane

    def beside(j):
        x_to = 1 - x_at if j % 2 else x_at
        y_to = 1 - y_at if j // 2 else y_at
        return y_to * 2 + x_to

    def in_plane(j):
        return level * 4 + beside(j)

    barrier = pltpu.get_barrier_semaphore()
    partners = [{"section": 1 - section}]
    partners += [{"expert": at_level(z)} for z in (mate, far_inner, far_outer)]
    partners += [{"expert": in_plane(j)} for j in range(1, 4)]
    for partner in partners:
        pl.semaphore_signal(
            barrier, inc=1, device_id=partner, device_id_type=pl.DeviceIdType.MESH
        )

    dense_ref[...] = jnp.zeros(dense_ref.shape, jnp.float32)
    held_at = place_ref[...] + groups * section
    holder_of = lax.broadcasted_iota(jnp.int32, (2 * groups, groups), 0)
    moves = jnp.where(holder_of == held_at, 1.0, 0.0).astype(jnp.bfloat16)
    expert_at = lax.broadcasted_iota(jnp.int32, (groups, rows), 0)
    for m in range(2):
        ids, route = ids_ref[m], route_ref[m]
        named = jnp.zeros((groups, rows), jnp.float32)
        for k in range(ids.shape[0]):
            named = jnp.where(ids[k : k + 1] == expert_at, route[k : k + 1], named)
        high = named.astype(jnp.bfloat16)
        low = (named - high.astype(jnp.float32)).astype(jnp.bfloat16)
        dense_ref[m, :, 0:rows] = sum(
            jnp.dot(moves, part, preferred_element_type=jnp.float32) for part in (high, low)
        )

    def scaled():
        values = hidden_ref[...]
        return values * lax.rsqrt(jnp.mean(values * values, axis=-1, keepdims=True) + EPSILON)

    hidden_ref[...] = tokens_ref[section].astype(jnp.float32)
    first_scaled = scaled()
    pl.semaphore_wait(barrier, len(partners))

    started, inner_only = [], []

    def remote(source, target, send_sem, arrival_sem, **peer):
        return pltpu.make_async_remote_copy(
            src_ref=source,
            dst_ref=target,
            send_sem=send_sem,
            recv_sem=arrival_sem,
            device_id=peer,
            device_id_type=pl.DeviceIdType.MESH,
        )

    def send(*ends, **peer):
        copy = remote(*ends, **peer)
        copy.start()
        started.append(copy)
        return copy

    def wait_for(target, arrival_sem):
        remote(target, target, arrival_sem, arrival_sem, expert=at_level(mate)).wait_recv()

    def to_core(i, source, target):
        return send(source, target, core_sends.at[i], core_arrivals.at[i], section=1 - section)

    gain_copy = to_core(0, gain_ref, other_gain)
    dense_copy = to_core(1, dense_ref.at[1 - section], other_dense)
    mats = [(gate_hbm, gate_mats), (up_hbm, up_mats), (down_hbm, down_mats)]
    mat_copies = [
        to_core(2 + i, source, target.at[section]) for i, (source, target) in enumerate(mats)
    ]
    own_copies = [
        pltpu.make_async_copy(source, target.at[section], core_sends.at[6 + i])
        for i, (source, target) in enumerate(mats)
    ]
    for copy in own_copies:
        copy.start()

    dense_copy.wait_recv()
    meta[0] = dense_ref[section] + other_dense[...]
    z_slots = [(mate, 1), (far_inner, 2 + outer), (far_outer, 2 + outer)]
    for i, (z, slot) in enumerate(z_slots):
        send(meta.at[0], meta.at[slot], meta_sends.at[i], meta_arrivals.at[slot], expert=at_level(z))
    for j in range(1, 4):
        place = 3 + j
        send(
            meta.at[0],
            meta.at[place],
            meta_sends.at[place],
            meta_arrivals.at[place],
            expert=in_plane(j),
        )
    gain_copy.wait_recv()
    is_first = section == 0
    gains = [
        jnp.where(is_first, gain_ref[...], other_gain[...]),
        jnp.where(is_first, other_gain[...], gain_ref[...]),
    ]

    span = meta.shape[2]
    row_at = lax.broadcasted_iota(jnp.int32, (span, span), 0)
    col_at = lax.broadcasted_iota(jnp.int32, (span, span), 1)
    earlier = jnp.where(row_at < col_at, 1.0, 0.0).astype(jnp.bfloat16)
    slot_at = lax.broadcasted_iota(jnp.int32, (4 * cap, rows), 0).astype(jnp.float32)
    plane_experts = [in_plane(j) for j in range(4)]
    column_experts = [at_level(z) for z in (level, mate, far_inner, far_outer)]

    def place_slots(place):
        if place:
            wait_for(meta.at[place], meta_arrivals.at[place])
        chosen = meta[place] > 0.0
        flags = jnp.where(chosen, 1.0, 0.0).astype(jnp.bfloat16)
        before = jnp.dot(flags, earlier, preferred_element_type=jnp.float32)
        places[place] = jnp.where(chosen, before, -512.0)

    def spread_over(place, experts, layer, weighted):
        spread = jnp.zeros((4 * cap, rows), jnp.float32)
        for j, expert in enumerate(experts):
            row = pl.ds(layer * 4 * depth + expert, 1)
            slot = places[place, row, 0:rows]
            value = meta[place, row, 0:rows] if weighted else 1.0
            spread = jnp.where(slot_at == slot + float(j * cap), value, spread)
        return spread

    def take(place, experts, layer, block):
        return jnp.dot(
            spread_over(place, experts, layer, False).astype(jnp.bfloat16),
            block,
            preferred_element_type=jnp.float32,
        ).astype(jnp.bfloat16)

    def scatter(place, experts, layer, returned_rows):
        spread = spread_over(place, experts, layer, True)
        high = spread.astype(jnp.bfloat16)
        low = (spread - high.astype(jnp.float32)).astype(jnp.bfloat16)
        both = lax.dot_general(
            jnp.concatenate([high, low], axis=1),
            returned_rows.reshape(4 * cap, returned_rows.shape[-1]),
            (((0,), (0,)), ((), ())),
            preferred_element_type=jnp.float32,
        )
        return both[0:rows] + both[rows:]

    for layer in range(2):
        start = first_scaled if layer == 0 else scaled()
        start = (start * gains[layer]).astype(jnp.bfloat16)
        blocks[layer, 0] = start[:, 0:main]
        flats[layer, 0] = start[:, main:]

        def block_copy(i, source, slot, z):
            return remote(
                blocks.at[layer, source],
                blocks.at[layer, slot],
                block_sends.at[layer, i],
                block_arrivals.at[layer, slot],
                expert=at_level(z),
            )

        for copy in (block_copy(0, 0, 1, mate), block_copy(1, 0, 2 + outer, far_inner)):
            copy.start()
            started.append(copy)
        flat_copies = [None] + [
            send(
                flats.at[layer, 0],
                flats.at[layer, j],
                flat_sends.at[layer, j],
                flat_arrivals.at[layer, j],
                expert=in_plane(j),
            )
            for j in range(1, 4)
        ]
        picked, returned, flat_home = {}, {}, {}

        def block_arrived(k):
            wait_for(blocks.at[layer, k], block_arrivals.at[layer, k])

        def pass_on():
            forwards = [block_copy(k, k, k, mate) for k in (2, 3)]
            inner_only.extend(forwards)

            @pl.when(outer == 0)
            def _():
                for k, forward in zip((2, 3), forwards):
                    block_arrived(k)
                    forward.start()

        def select(k):
            if layer == 0:
                place_slots(k)
            if k == 1:
                block_arrived(k)
            if k >= 2:
                pl.when(outer == 1)(functools.partial(block_arrived, k))
            taken = take(k, plane_experts, layer, blocks[layer, k])
            for j in range(1, 4):
                picks[layer, k, j] = taken[j * cap : (j + 1) * cap]
                picked[k, j] = send(
                    picks.at[layer, k, j],
                    held.at[layer, k, j],
                    pick_sends.at[layer, k, j],
                    pick_arrivals.at[layer, k, j],
                    expert=in_plane(j),
                )
            held[layer, k, 0] = taken[0:cap]

        def select_flat(j):
            place = 3 + j if j else 0
            if j:
                if layer == 0:
                    place_slots(place)
                flat_copies[j].wait_recv()
            taken = take(place, column_experts, layer, flats[layer, j])
            for i, (z, slot) in enumerate(z_slots):
                flat_picks[layer, j, i] = taken[(i + 1) * cap : (i + 2) * cap]
                send(
                    flat_picks.at[layer, j, i],
                    flat_held.at[layer, slot, j],
                    flat_pick_sends.at[layer, j, i],
                    flat_pick_arrivals.at[layer, slot, j],
                    expert=at_level(z),
                )
            flat_held[layer, 0, j] = taken[0:cap]

        def compute(k):
            for j in range(1, 4):
                picked[k, j].wait_recv()
            if k:
                for j in range(4):
                    wait_for(flat_held.at[layer, k, j], flat_pick_arrivals.at[layer, k, j])
            block = held[layer, k].reshape(4 * cap, main)
            rest = flat_held[layer, k].reshape(4 * cap, width - main)

            def project(mats):
                return jnp.dot(
                    block, mats[layer, 0:main], preferred_element_type=jnp.float32
                ) + jnp.dot(rest, mats[layer, main:], preferred_element_type=jnp.float32)

            gate_part = project(gate_mats)
            up_part = project(up_mats)
            hidden_units = (gate_part / (1.0 + jnp.exp(-gate_part)) * up_part).astype(
                jnp.bfloat16
            )
            out = jnp.dot(hidden_units, down_mats[layer], preferred_element_type=jnp.float32)
            out = out.astype(jnp.bfloat16)
            for j in range(1, 4):
                outs[layer, k, j] = out[j * cap : (j + 1) * cap, 0:back]
                returned[k, j] = send(
                    outs.at[layer, k, j],
                    rets.at[layer, k, j],
                    ret_sends.at[layer, k, j],
                    ret_arrivals.at[layer, k, j],
                    expert=in_plane(j),
                )
            rets[layer, k, 0] = out[0:cap, 0:back]
            flat_out = out[:, back:].reshape(4, cap, width - back)
            if k:
                flat_outs[layer, k - 1] = flat_out
                z, slot = z_slots[k - 1]
                send(
                    flat_outs.at[layer, k - 1],
                    flat_rets.at[layer, slot],
                    flat_ret_sends.at[layer, k],
                    flat_ret_arrivals.at[layer, slot],
                    expert=at_level(z),
                )
            else:
                flat_rets[layer, 0] = flat_out

        def combine(k):
            for j in range(1, 4):
                returned[k, j].wait_recv()
            return scatter(k, plane_experts, layer, rets[layer, k])

        def combine_flat(j):
            place = 3 + j if j else 0
            return scatter(place, column_experts, layer, flat_rets[layer, :, j])

        def send_home(k, target, arrival, z):
            copy = remote(
                sums.at[layer, k], target, home_sends.at[layer, k], arrival, expert=at_level(z)
            )
            copy.start()
            return copy

        def combine_far(k):
            part = combine(k)

            @pl.when(outer == 1)
            def _():
                sums[layer, k] = part.astype(jnp.bfloat16)
                relay, arrival = relays.at[layer, k - 2], relay_arrivals.at[layer, k - 2]
                send_home(k, relay, arrival, mate)

            @pl.when(outer == 0)
            def _():
                parts[k - 2] = part

        def join_far(k):
            @pl.when(outer == 0)
            def _():
                wait_for(relays.at[layer, k - 2], relay_arrivals.at[layer, k - 2])
                joined = parts[k - 2] + relays[layer, k - 2].astype(jnp.float32)
                sums[layer, k] = joined.astype(jnp.bfloat16)
                z = far_inner if k == 2 else far_outer
                send_home(k, homes.at[layer, 1], home_arrivals.at[layer, 1], z)

        select(0)
        select(1)
        pass_on()
        select(2)
        select_flat(0)
        select_flat(1)
        select_flat(2)
        select_flat(3)
        select(3)
        if layer == 0:
            for copy in own_copies:
                copy.wait()
            for copy in mat_copies:
                copy.wait_recv()
        for k in (2, 3, 1, 0):
            compute(k)
        combine_far(2)
        combine_far(3)
        sums[layer, 1] = combine(1).astype(jnp.bfloat16)
        started.append(send_home(1, homes.at[layer, 0], home_arrivals.at[layer, 0], mate))
        for k in range(1, depth):
            wait_for(flat_rets.at[layer, k], flat_ret_arrivals.at[layer, k])
        for j in range(1, 4):
            flat_sums[layer, j] = combine_flat(j).astype(jnp.bfloat16)
            flat_home[j] = send(
                flat_sums.at[layer, j],
                flat_homes.at[layer, j],
                flat_home_sends.at[layer, j],
                flat_home_arrivals.at[layer, j],
                expert=in_plane(j),
            )
        join_far(2)
        flat_mixture = combine_flat(0)
        join_far(3)
        mixture = combine(0)
        for j in range(1, 4):
            flat_home[j].wait_recv()
            flat_mixture = flat_mixture + flat_homes[layer, j].astype(jnp.float32)
        for i in range(2):
            wait_for(homes.at[layer, i], home_arrivals.at[layer, i])
            mixture = mixture + homes[layer, i].astype(jnp.float32)
        mixed = jnp.concatenate([mixture, flat_mixture], axis=1)
        hidden = (hidden_ref[...] + mixed).astype(jnp.bfloat16)
        if layer == 0:
            hidden_ref[...] = hidden.astype(jnp.float32)
        else:
            finals[0] = hidden

    final_copy = to_core(5, finals.at[0], finals.at[1])
    final_copy.wait_recv()
    for layer in range(2):
        for k in (2, 3):
            done = home_sends.at[layer, k]
            started.append(remote(sums.at[layer, k], sums.at[layer, k], done, done, expert=at_level(mate)))
    for copy in started:
        copy.wait_send()

    @pl.when(outer == 0)
    def _():
        for copy in inner_only:
            copy.wait_send()


def cascade_call(
    tokens, gain, place, ids, route, gate_matrix, up_matrix, down_matrix, depth, cap
):
    rows, width = tokens.shape[1:]
    table = (8 * depth, rows + -rows % 128)
    main = width - width // 4 // 128 * 128
    back = width - 3 * width // 16 // 128 * 128
    vmem = pl.BlockSpec(memory_space=pltpu.VMEM)
    anywhere = pl.BlockSpec(memory_space=pl.ANY)
    bf16, f32 = jnp.bfloat16, jnp.float32
    sems = pltpu.SemaphoreType.DMA
    return pl.pallas_call(
        functools.partial(cascade_kernel, depth, cap),
        out_shape=jax.ShapeDtypeStruct((2, rows, width), bf16),
        in_specs=[vmem] * 5 + [anywhere] * 3,
        out_specs=vmem,
        scratch_shapes=[
            pltpu.VMEM((2,) + gate_matrix.shape, bf16),
            pltpu.VMEM((2,) + up_matrix.shape, bf16),
            pltpu.VMEM((2,) + down_matrix.shape, bf16),
            pltpu.VMEM(gain.shape, f32),
            pltpu.VMEM(table, f32),
            pltpu.VMEM((depth + 3,) + table, f32),
            pltpu.VMEM((depth + 3,) + table, f32),
            pltpu.VMEM((2, depth, rows, main), bf16),
            pltpu.VMEM((2, depth, 4, cap, main), bf16),
            pltpu.VMEM((2, depth, 4, cap, main), bf16),
            pltpu.VMEM((2, depth, 4, cap, back), bf16),
            pltpu.VMEM((2, depth, 4, cap, back), bf16),
            pltpu.VMEM((2, depth, rows, back), bf16),
            pltpu.VMEM((2, 2, rows, back), bf16),
            pltpu.VMEM((2, 2, rows, back), bf16),
            pltpu.VMEM((2, 4, rows, width - main), bf16),
            pltpu.VMEM((2, 4, depth - 1, cap, width - main), bf16),
            pltpu.VMEM((2, depth, 4, cap, width - main), bf16),
            pltpu.VMEM((2, depth - 1, 4, cap, width - back), bf16),
            pltpu.VMEM((2, depth, 4, cap, width - back), bf16),
            pltpu.VMEM((2, 4, rows, width - back), bf16),
            pltpu.VMEM((2, 4, rows, width - back), bf16),
            pltpu.VMEM((2, rows, back), f32),
            pltpu.VMEM((rows, width), f32),
            pltpu.VMEM((2,) + table, f32),
            sems((9,)),
            sems((6,)),
            sems((depth + 3,)),
            sems((depth + 3,)),
            sems((2, depth)),
            sems((2, depth)),
            sems((2, depth, 4)),
            sems((2, depth, 4)),
            sems((2, depth, 4)),
            sems((2, depth, 4)),
            sems((2, depth)),
            sems((2, 2)),
            sems((2, 2)),
            sems((2, 4)),
            sems((2, 4)),
            sems((2, 4, depth - 1)),
            sems((2, depth, 4)),
            sems((2, depth)),
            sems((2, depth)),
            sems((2, 4)),
            sems((2, 4)),
        ],
        compiler_params=pltpu.CompilerParams(
            collective_id=0,
            has_side_effects=True,
            vmem_limit_bytes=60 * 1024 * 1024,
        ),
    )(tokens, gain, place, ids, route, gate_matrix, up_matrix, down_matrix)


def dense_local(
    tokens, norm_gain, gate_weight, up_weight, down_weight, expert_place, expert_ids, route_weights
):
    groups = lax.axis_size("expert")
    section_index = lax.axis_index("section")
    tok_rows, top_count = expert_ids.shape[2:]
    cap = 5 * tok_rows * top_count // (4 * groups)
    finals = cascade_call(
        tokens,
        norm_gain,
        expert_place,
        jnp.swapaxes(expert_ids[0], 1, 2),
        jnp.swapaxes(route_weights[0], 1, 2),
        gate_weight[0, 0],
        up_weight[0, 0],
        down_weight[0, 0],
        groups // 4,
        cap,
    )
    return jnp.where(section_index == 0, finals, finals[::-1])


def local(
    tokens, norm_gain, gate_weight, up_weight, down_weight, expert_place, expert_ids, route_weights
):
    dense = 2 * expert_ids.shape[3] >= expert_place.shape[1] and tokens.shape[0] == 2
    dense = dense and lax.axis_size("expert") % 4 == 0 and lax.axis_size("expert") == 16
    run = dense_local if dense else routed_local
    return run(
        tokens,
        norm_gain,
        gate_weight,
        up_weight,
        down_weight,
        expert_place,
        expert_ids,
        route_weights,
    )


def solution(mesh):
    in_specs = (
        P(None, "expert", None),
        P("section", None),
        P("section", "expert", None, None),
        P("section", "expert", None, None),
        P("section", "expert", None, None),
        P("section", None),
        P("section", None, "expert", None),
        P("section", None, "expert", None),
    )
    out_specs = P(None, "expert", None)
    return jax.shard_map(local, mesh=mesh, in_specs=in_specs, out_specs=out_specs, check_vma=False)
```
